32 devices in a mesh: tm: 4 (over z), ent: 2 (over y), batch: 4 (over x, core).
Axes of the slice: x: 2, y: 2, z: 4, core: 2. Of those that a mesh axis runs over, the one named last changes fastest.
Arguments:
- init_state: float32 [4, 1024, 256], P('batch', 'ent'), may hold values from -6 to 6
- tiles: float32 [4, 4, 4, 512, 512], P('batch', 'tm', 'ent'), may hold values from -0.25 to 0.25
- dst_block: int32 [4, 4, 4], P('batch', 'tm', 'ent'), may hold values from 0 to 1
- rel_id: int32 [4, 4, 4], P('batch', 'tm', 'ent'), may hold values from 0 to 255
- cotangent: float32 [4, 4, 1024, 256], P('batch', 'tm', 'ent'), may hold values from -0.125 to 0.125
- rel_emb: float32 [256, 256], replicated, may hold values from -6 to 6
- w_neigh: float32 [256, 256], replicated, may hold values from -0.1875 to 0.1875
- w_self: float32 [256, 256], replicated, may hold values from -0.375 to 0.375
- w_gate: float32 [256, 256], replicated, may hold values from -0.375 to 0.375
- b_gate: float32 [256], replicated, may hold values from -2 to 2
Outputs:
- states: float32 [4, 4, 1024, 256], P('batch', 'tm', 'ent')
- grad_rel: float32 [256, 256], replicated
- grad_neigh: float32 [256, 256], replicated
- grad_self: float32 [256, 256], replicated
- grad_gate: float32 [256, 256], replicated
- grad_bias: float32 [256], replicated
The draws below stay inside these ranges and needn't reach their ends.
All inputs are finite; a program needn't handle non-finite values.
Results may differ from the reference program's by a relative error of at most 0.00012.
Values sent between devices are 32-bit elements; how exact they have to be, the bound alone decides.
A program may use at most 64 MiB of HBM per device.

```python
import jax
import jax.numpy as jnp
from jax import lax

D = 256
REL = 256
TILE = 512
TILES_DEV = 2
SNAPS = 4
ENTITIES = 1024
BLOCKS_ALL = 4
WINDOWS = 4
N_ENT = 2
N_BATCH = 4


def set_ends(values, own_key, smallest, high):
    place = [jax.random.randint(jax.random.fold_in(own_key, axis), (), 0, length) for axis, length in enumerate(values.shape)]
    longest = values.shape.index(max(values.shape))
    neighbour = place[:longest] + [(place[longest] + 1) % values.shape[longest]] + place[longest + 1:]
    return values.at[tuple(place)].set(smallest).at[tuple(neighbour)].set(high)


def level_of(rng, shape, cuts, least, high):
    def one(position, blocks):
        draws = jax.random.uniform(jax.random.fold_in(jax.random.fold_in(rng, 6), position), (blocks,), jnp.float32, least / len(cuts), high / len(cuts))
        return jnp.repeat(jnp.exp(draws), shape[position] // blocks).reshape((-1,) + (1,) * (len(shape) - position - 1))

    loudness = one(*cuts[0])
    for cut in cuts[1:]:
        loudness = loudness * one(*cut)
    return loudness


def bell_draw(stream_key, shape, deviation, most, split=(), kind=jnp.bfloat16):
    array = jax.random.normal(stream_key, shape, jnp.float32) * deviation
    if len(split) > 0:
        array = level_of(stream_key, shape, split, -0.22, 0.18) * array
    return jnp.clip(array, min=-most, max=most).astype(kind)


def setup_inputs(seed: int = 0) -> dict:
    arg_keys = jax.random.split(jax.random.key(seed), 11)
    return {
        "init_state": bell_draw(arg_keys[0], (WINDOWS, ENTITIES, D), 1.0, 6.0, ((0, 4), (1, 2)), jnp.float32),
        "tiles": bell_draw(arg_keys[1], (WINDOWS, SNAPS, BLOCKS_ALL, TILE, TILE), TILE ** -0.5, 0.25, ((0, 4), (1, 4), (2, 2)), jnp.float32),
        "dst_block": set_ends(jax.random.randint(arg_keys[2], (WINDOWS, SNAPS, BLOCKS_ALL), 0, N_ENT), jax.random.fold_in(arg_keys[2], 1), 0, N_ENT - 1).astype(jnp.int32),
        "rel_id": set_ends(jax.random.randint(arg_keys[3], (WINDOWS, SNAPS, BLOCKS_ALL), 0, REL), jax.random.fold_in(arg_keys[3], 1), 0, REL - 1).astype(jnp.int32),
        "cotangent": bell_draw(arg_keys[4], (WINDOWS, SNAPS, ENTITIES, D), (1.0 / (SNAPS * ENTITIES * N_BATCH) ** 0.5), 0.125, ((0, 4), (1, 4), (2, 2)), jnp.float32),
        "rel_emb": bell_draw(arg_keys[5], (REL, D), 1.0, 6.0, (), jnp.float32),
        "w_neigh": bell_draw(arg_keys[6], (D, D), (4 * D) ** -0.5, 0.1875, (), jnp.float32),
        "w_self": bell_draw(arg_keys[7], (D, D), D ** -0.5, 0.375, (), jnp.float32),
        "w_gate": bell_draw(arg_keys[8], (D, D), D ** -0.5, 0.375, (), jnp.float32),
        "b_gate": jnp.clip(jax.random.uniform(arg_keys[9], (D,), jnp.float32, -2.0, 2.0), -2.0, 2.0),
    }


highest = lax.Precision.HIGHEST

def snapshot(current, tiles_t, dst_t, rel_t, params):
    rel_emb, w_neigh, w_self, w_gate, b_gate = params
    held_rows = current.reshape(N_ENT, TILE, D)
    owner_block = jnp.arange(N_ENT * TILES_DEV, dtype=jnp.int32) // TILES_DEV
    source = held_rows[owner_block]
    rows_sum = lax.optimization_barrier(jnp.sum(tiles_t, axis=2))
    result = jnp.einsum('tij,tjd->tid', tiles_t, source, precision=highest)
    result = result + rows_sum[:, :, None] * rel_emb[rel_t][:, None, :]
    dest_pick = (dst_t[:, None] == jnp.arange(N_ENT, dtype=jnp.int32)[None, :]).astype(jnp.float32)
    incoming = jnp.einsum('tg,tid->gid', dest_pick, result, precision=highest).reshape(ENTITIES, D)
    update_gate = jax.nn.sigmoid(jnp.dot(current, w_gate, precision=highest) + b_gate)
    candidate = jnp.tanh(jnp.dot(incoming, w_neigh, precision=highest) + jnp.dot(current, w_self, precision=highest))
    return update_gate * candidate + (1.0 - update_gate) * current

def reference(init_state, tiles, dst_block, rel_id, cotangent, rel_emb, w_neigh, w_self, w_gate, b_gate):
    params = (rel_emb, w_neigh, w_self, w_gate, b_gate)
    all_states = []
    totals = None
    for window in range(WINDOWS):

        def run_window(weights):
            current = init_state[window]
            collected = []
            for snap_index in range(SNAPS):
                current = snapshot(current, tiles[window, snap_index], dst_block[window, snap_index], rel_id[window, snap_index], weights)
                collected.append(current)
            return jnp.stack(collected)
        outputs, pullback = jax.vjp(run_window, params)
        grads_now = pullback(cotangent[window])[0]
        all_states.append(outputs)
        if totals is None:
            totals = grads_now
        else:
            totals = tuple((a + b for a, b in zip(totals, grads_now)))
    return (jnp.stack(all_states), totals[0], totals[1], totals[2], totals[3], totals[4])
```

```python
import functools

import jax
import jax.numpy as jnp
from jax import lax
from jax.experimental import pallas as pl
from jax.experimental.pallas import tpu as pltpu
from jax.sharding import PartitionSpec as P

MESH = pl.DeviceIdType.MESH
CHUNKS = 4
f32, bf16 = jnp.float32, jnp.bfloat16
NN = (((1,), (0,)), ((), ()))
NT = (((1,), (1,)), ((), ()))


def split(value):
    high = value.astype(bf16)
    return high, (value - high.astype(f32)).astype(bf16)


def dot3(left, right, dims=NN):
    one = functools.partial(
        lax.dot_general, dimension_numbers=dims, preferred_element_type=f32
    )
    return one(left[0], right[0]) + (one(left[0], right[1]) + one(left[1], right[0]))


def remote(src, dst, send, recv, axis, index):
    return pltpu.make_async_remote_copy(
        src_ref=src, dst_ref=dst, send_sem=send, recv_sem=recv,
        device_id={axis: index}, device_id_type=MESH,
    )


def step_kernel(
    n_tm, n_ent,
    dst_ref, rel_ref, init_ref, tiles_ref, cot_ref, emb_ref, wn_ref, ws_ref, wg_ref, bias_ref,
    states_ref, grel_ref, gneigh_ref, gself_ref, ggate_ref, gbias_ref,
    st, dz, dout, agg, upd, cand, proj, part, ysend, yrecv, dagg, grecv, msg_out, msg_in,
    th, tl, tth, ttl, wnh, wnl, wsh, wsl, wgh, wgl, sth, stl, agh, agl, coef_a, coef_b,
    dpre, dgate, dprev,
    ys_sem, yr_sem, gs_sem, gr_sem, ms_sem, mr_sem, zs_sem, zr_sem, bs_sem, br_sem,
):
    tm = lax.axis_index("tm")
    ent = lax.axis_index("ent")
    n_tile = tiles_ref.shape[0]
    rows, width = init_ref.shape
    step = rows // CHUNKS
    chunk = [slice(c * step, (c + 1) * step) for c in range(CHUNKS)]
    peers = [lax.rem(ent + off, n_ent) for off in range(n_ent)]
    up = jnp.minimum(tm + 1, n_tm - 1)
    down = jnp.maximum(tm - 1, 0)
    has_up, has_down = tm < n_tm - 1, tm > 0

    barrier = pltpu.get_barrier_semaphore()
    for off in range(1, n_ent):
        pl.semaphore_signal(barrier, inc=1, device_id={"ent": peers[off]}, device_id_type=MESH)

    @pl.when(has_up)
    def _():
        pl.semaphore_signal(barrier, inc=1, device_id={"tm": up}, device_id_type=MESH)

    @pl.when(has_down)
    def _():
        pl.semaphore_signal(barrier, inc=1, device_id={"tm": down}, device_id_type=MESH)

    for k in range(n_tile):
        th[k], tl[k] = split(tiles_ref[k])
    wnh[...], wnl[...] = split(wn_ref[...])
    wsh[...], wsl[...] = split(ws_ref[...])
    wgh[...], wgl[...] = split(wg_ref[...])
    wn, ws, wg = (wnh, wnl), (wsh, wsl), (wgh, wgl)

    def both(pair, *index):
        return tuple(ref[index] if index else ref[...] for ref in pair)

    @pl.when(tm == 0)
    def _():
        st[...] = init_ref[...]

    @pl.when(tm == n_tm - 1)
    def _():
        dz[...] = jnp.zeros_like(dz)

    pl.semaphore_wait(
        barrier, n_ent - 1 + has_up.astype(jnp.int32) + has_down.astype(jnp.int32)
    )

    hits = [
        [(dst_ref[k] == peers[off]).astype(f32) for k in range(n_tile)] for off in range(n_ent)
    ]
    rel_rows = [emb_ref[pl.ds(rel_ref[k], 1), :] for k in range(n_tile)]
    row_sums = [jnp.sum(tiles_ref[k], axis=1, keepdims=True) for k in range(n_tile)]
    for k in range(n_tile):
        part[k] = row_sums[k] * rel_rows[k]

    def y_copy(off, c):
        return remote(
            ysend.at[off - 1, chunk[c]], yrecv.at[off - 1, chunk[c]],
            ys_sem.at[off - 1, c], yr_sem.at[off - 1, c], "ent", peers[off],
        )

    def z_copy(c):
        return remote(
            states_ref.at[chunk[c]], st.at[chunk[c]], zs_sem.at[c], zr_sem.at[c], "tm", up
        )

    def project(c, pieces):
        proj[0, chunk[c]] = dot3(pieces, both(wg))
        proj[1, chunk[c]] = dot3(pieces, both(ws))

    for c in range(CHUNKS):

        @pl.when(has_down)
        def _():
            z_copy(c).wait_recv()

        pieces = split(st[chunk[c]])
        if c < CHUNKS - 1:
            for k in range(n_tile):
                part[k] += dot3(both((th, tl), k, slice(None), chunk[c]), pieces)
            project(c, pieces)
        else:
            for d in range(CHUNKS):
                done = [
                    part[k, chunk[d]] + dot3(both((th, tl), k, chunk[d], chunk[c]), pieces)
                    for k in range(n_tile)
                ]
                for off in range(1, n_ent):
                    ysend[off - 1, chunk[d]] = sum(
                        done[k] * hits[off][k] for k in range(n_tile)
                    )
                    y_copy(off, d).start()
                agg[chunk[d]] = sum(done[k] * hits[0][k] for k in range(n_tile))
            project(c, pieces)

    for c in range(CHUNKS):
        total = agg[chunk[c]]
        for off in range(1, n_ent):
            y_copy(off, c).wait_recv()
            total = total + yrecv[off - 1, chunk[c]]
        agg[chunk[c]] = total
        u = jax.nn.sigmoid(proj[0, chunk[c]] + bias_ref[...])
        v = jnp.tanh(dot3(split(total), both(wn)) + proj[1, chunk[c]])
        states_ref[chunk[c]] = u * v + (1.0 - u) * st[chunk[c]]

        @pl.when(has_up)
        def _():
            z_copy(c).start()

        upd[chunk[c]] = u
        cand[chunk[c]] = v

    for k in range(n_tile):
        turned = tiles_ref[k].T
        sums = jnp.sum(turned, axis=0, keepdims=True)
        tth[k], ttl[k] = split(turned)
        for off in range(n_ent):
            target = msg_in if off == 0 else msg_out
            target[off, k : k + 1] = sums * hits[off][k]
            target[off, n_tile + k : n_tile + k + 1] = jnp.full_like(
                sums, rel_ref[k].astype(f32)
            )
    for off in range(n_ent):
        target = msg_in if off == 0 else msg_out
        if target.shape[1] > 2 * n_tile:
            target[off, 2 * n_tile :] = jnp.zeros(
                (target.shape[1] - 2 * n_tile, target.shape[2]), f32
            )

    def m_copy(off):
        return remote(
            msg_out.at[off], msg_in.at[off], ms_sem.at[off - 1], mr_sem.at[off - 1],
            "ent", peers[off],
        )

    for off in range(1, n_ent):
        m_copy(off).start()
    sth[...], stl[...] = split(st[...].T)
    agh[...], agl[...] = split(agg[...].T)
    u, v = upd[...], cand[...]
    coef_a[...] = u * (1.0 - v * v)
    coef_b[...] = (v - st[...]) * u * (1.0 - u)

    def g_copy(off, c):
        return remote(
            dagg.at[chunk[c]], grecv.at[off - 1, chunk[c]],
            gs_sem.at[off - 1, c], gr_sem.at[off - 1, c], "ent", peers[off],
        )

    def b_copy(c):
        return remote(dout.at[chunk[c]], dz.at[chunk[c]], bs_sem.at[c], br_sem.at[c], "tm", down)

    for c in range(CHUNKS):

        @pl.when(has_up)
        def _():
            b_copy(c).wait_recv()

        dnew = dz[chunk[c]] + cot_ref[chunk[c]]
        pre = dnew * coef_a[chunk[c]]
        gate = dnew * coef_b[chunk[c]]
        pre_pieces = split(pre)
        dagg[chunk[c]] = dot3(pre_pieces, both(wn), NT)

        @pl.when(has_down)
        def _():
            for off in range(1, n_ent):
                g_copy(off, c).start()

        dpre[chunk[c]] = pre
        dgate[chunk[c]] = gate

        @pl.when(has_down)
        def _():
            dprev[chunk[c]] = (
                dnew * (1.0 - upd[chunk[c]])
                + dot3(pre_pieces, both(ws), NT)
                + dot3(split(gate), both(wg), NT)
            )

    @pl.when(has_down)
    def _():
        for c in range(CHUNKS):
            own = dagg[chunk[c]]
            spread = [own * hits[0][k] for k in range(n_tile)]
            for off in range(1, n_ent):
                g_copy(off, c).wait_recv()
                other = grecv[off - 1, chunk[c]]
                for k in range(n_tile):
                    spread[k] = spread[k] + other * hits[n_ent - off][k]
            pieces = [split(spread[k]) for k in range(n_tile)]
            if c < CHUNKS - 1:
                dprev[...] += sum(
                    dot3(both((tth, ttl), k, slice(None), chunk[c]), pieces[k])
                    for k in range(n_tile)
                )
            else:
                for d in range(CHUNKS):
                    dout[chunk[d]] = dprev[chunk[d]] + sum(
                        dot3(both((tth, ttl), k, chunk[d], chunk[c]), pieces[k])
                        for k in range(n_tile)
                    )
                    b_copy(d).start()

    pre_pieces, gate_pieces = split(dpre[...]), split(dgate[...])
    gneigh_ref[...] = dot3(both((agh, agl)), pre_pieces)
    gself_ref[...] = dot3(both((sth, stl)), pre_pieces)
    ggate_ref[...] = dot3(both((sth, stl)), gate_pieces)
    gbias_ref[...] = jnp.sum(dgate[...], axis=0, keepdims=True)
    grad_pieces = split(dagg[...])
    number = lax.broadcasted_iota(jnp.int32, grel_ref.shape, 0).astype(f32)
    grad_rel = jnp.zeros(grel_ref.shape, f32)
    for off in range(n_ent):
        if off > 0:
            m_copy(off).wait_recv()
        found = dot3(split(msg_in[off]), grad_pieces)
        for k in range(n_tile):
            place = msg_in[off, n_tile + k : n_tile + k + 1, 0:1]
            grad_rel = grad_rel + jnp.where(number == place, found[k : k + 1], 0.0)
    grel_ref[...] = grad_rel

    for off in range(1, n_ent):
        m_copy(off).wait_send()
        for c in range(CHUNKS):
            y_copy(off, c).wait_send()

    @pl.when(has_up)
    def _():
        for c in range(CHUNKS):
            z_copy(c).wait_send()

    @pl.when(has_down)
    def _():
        for c in range(CHUNKS):
            b_copy(c).wait_send()
            for off in range(1, n_ent):
                g_copy(off, c).wait_send()


def on_device(
    n_tm, n_ent,
    init_state, tiles, dst_block, rel_id, cotangent, rel_emb, w_neigh, w_self, w_gate, b_gate
):
    assert tiles.shape[:2] == (1, 1)
    n_tile, rows = tiles.shape[2], tiles.shape[3]
    width, n_rel = init_state.shape[2], rel_emb.shape[0]
    lines = -(-2 * n_tile // 8) * 8
    others = max(n_ent - 1, 1)
    square, flat = (n_tile, rows, rows), (rows, width)
    vmem = pltpu.VMEM
    sems = pltpu.SemaphoreType.DMA
    whole, small = pl.BlockSpec(memory_space=pltpu.VMEM), pl.BlockSpec(memory_space=pltpu.SMEM)
    shape = lambda *dims: jax.ShapeDtypeStruct(dims, f32)
    weight = (width, width)
    outs = pl.pallas_call(
        functools.partial(step_kernel, n_tm, n_ent),
        out_shape=(
            shape(rows, width), shape(n_rel, width), shape(*weight), shape(*weight),
            shape(*weight), shape(1, width),
        ),
        in_specs=[small, small] + [whole] * 8,
        out_specs=(whole,) * 6,
        scratch_shapes=[
            vmem(flat, f32), vmem(flat, f32), vmem(flat, f32), vmem(flat, f32),
            vmem(flat, f32), vmem(flat, f32), vmem((2,) + flat, f32),
            vmem((n_tile,) + flat, f32),
            vmem((others,) + flat, f32), vmem((others,) + flat, f32),
            vmem(flat, f32), vmem((others,) + flat, f32),
            vmem((n_ent, lines, rows), f32), vmem((n_ent, lines, rows), f32),
            vmem(square, bf16), vmem(square, bf16), vmem(square, bf16), vmem(square, bf16),
            vmem(weight, bf16), vmem(weight, bf16), vmem(weight, bf16), vmem(weight, bf16),
            vmem(weight, bf16), vmem(weight, bf16),
            vmem((width, rows), bf16), vmem((width, rows), bf16),
            vmem((width, rows), bf16), vmem((width, rows), bf16),
            vmem(flat, f32), vmem(flat, f32), vmem(flat, f32), vmem(flat, f32), vmem(flat, f32),
            sems((others, CHUNKS)), sems((others, CHUNKS)),
            sems((others, CHUNKS)), sems((others, CHUNKS)),
            sems((others,)), sems((others,)),
            sems((CHUNKS,)), sems((CHUNKS,)), sems((CHUNKS,)), sems((CHUNKS,)),
        ],
        compiler_params=pltpu.CompilerParams(
            collective_id=0, has_side_effects=True, vmem_limit_bytes=60 * 1024 * 1024
        ),
    )(
        dst_block[0, 0], rel_id[0, 0], init_state[0], tiles[0, 0], cotangent[0, 0],
        rel_emb, w_neigh, w_self, w_gate, b_gate[None],
    )
    totals = lax.psum(outs[1:], ("tm", "ent", "batch"))
    return (outs[0][None, None], totals[0], totals[1], totals[2], totals[3], totals[4][0])


def solution(mesh):
    placed = (
        P("batch", "ent", None),
        P("batch", "tm", "ent", None, None),
        P("batch", "tm", "ent"),
        P("batch", "tm", "ent"),
        P("batch", "tm", "ent", None),
        P(),
        P(),
        P(),
        P(),
        P(),
    )
    return jax.shard_map(
        functools.partial(on_device, mesh.shape["tm"], mesh.shape["ent"]),
        mesh=mesh,
        in_specs=placed,
        out_specs=(P("batch", "tm", "ent", None), P(), P(), P(), P(), P()),
        check_vma=False,
    )
```

```python
import functools

import jax
import jax.numpy as jnp
from jax import lax
from jax.experimental import pallas as pl
from jax.experimental.pallas import tpu as pltpu
from jax.sharding import PartitionSpec as P

MESH = pl.DeviceIdType.MESH
CHUNKS = 4
f32, bf16 = jnp.float32, jnp.bfloat16
NN = (((1,), (0,)), ((), ()))
NT = (((1,), (1,)), ((), ()))


def split(value):
    high = value.astype(bf16)
    return high, (value - high.astype(f32)).astype(bf16)


def dot3(left, right, dims=NN):
    one = functools.partial(
        lax.dot_general, dimension_numbers=dims, preferred_element_type=f32
    )
    return one(left[0], right[0]) + (one(left[0], right[1]) + one(left[1], right[0]))


def remote(src, dst, send, recv, axis, index):
    return pltpu.make_async_remote_copy(
        src_ref=src, dst_ref=dst, send_sem=send, recv_sem=recv,
        device_id={axis: index}, device_id_type=MESH,
    )


def step_kernel(
    n_tm, n_ent, n_batch,
    dst_ref, rel_ref, init_ref, tiles_ref, cot_ref, emb_ref, wn_ref, ws_ref, wg_ref, bias_ref,
    states_ref, grel_ref, gneigh_ref, gself_ref, ggate_ref, gbias_ref,
    st, dz, dout, agg, upd, cand, proj, part, ysend, yrecv, dagg, grecv, msg_out, msg_in,
    th, tl, tth, ttl, wnh, wnl, wsh, wsl, wgh, wgl, sth, stl, agh, agl, coef_a, coef_b,
    dpre, dgate, dprev,
    grads, pair_in, half_sum, plane_in, chain_in, chain_out, final,
    ys_sem, yr_sem, gs_sem, gr_sem, ms_sem, mr_sem, zs_sem, zr_sem, bs_sem, br_sem,
    one_sem, rs_sem, rr_sem, cs_sem, as_sem, ar_sem,
):
    tm = lax.axis_index("tm")
    ent = lax.axis_index("ent")
    n_tile = tiles_ref.shape[0]
    rows, width = init_ref.shape
    step = rows // CHUNKS
    chunk = [slice(c * step, (c + 1) * step) for c in range(CHUNKS)]
    peers = [lax.rem(ent + off, n_ent) for off in range(n_ent)]
    up = jnp.minimum(tm + 1, n_tm - 1)
    down = jnp.maximum(tm - 1, 0)
    has_up, has_down = tm < n_tm - 1, tm > 0

    batch = lax.axis_index("batch")
    side = lax.rem(batch, 2)
    pair = {"batch": batch + 1 - 2 * side}
    members = n_batch // 2 * n_ent
    member = batch // 2 * n_ent + ent
    size = plane_in.shape[1]

    def mate(distance):
        index = lax.rem(member + distance + members, members)
        return index, {"batch": index // n_ent * 2 + side, "ent": lax.rem(index, n_ent)}

    barrier = pltpu.get_barrier_semaphore()
    for q in range(1, members):
        pl.semaphore_signal(barrier, inc=1, device_id=mate(q)[1], device_id_type=MESH)
    pl.semaphore_signal(barrier, inc=1, device_id=pair, device_id_type=MESH)
    for q in range(1, n_tm):
        pl.semaphore_signal(
            barrier, inc=1, device_id={"tm": lax.rem(tm + q, n_tm)}, device_id_type=MESH
        )

    for k in range(n_tile):
        th[k], tl[k] = split(tiles_ref[k])
    wnh[...], wnl[...] = split(wn_ref[...])
    wsh[...], wsl[...] = split(ws_ref[...])
    wgh[...], wgl[...] = split(wg_ref[...])
    wn, ws, wg = (wnh, wnl), (wsh, wsl), (wgh, wgl)

    def both(pair, *index):
        return tuple(ref[index] if index else ref[...] for ref in pair)

    @pl.when(tm == 0)
    def _():
        st[...] = init_ref[...]

    @pl.when(tm == n_tm - 1)
    def _():
        dz[...] = jnp.zeros_like(dz)

    pl.semaphore_wait(barrier, members + n_tm - 1)

    hits = [
        [(dst_ref[k] == peers[off]).astype(f32) for k in range(n_tile)] for off in range(n_ent)
    ]
    rel_rows = [emb_ref[pl.ds(rel_ref[k], 1), :] for k in range(n_tile)]
    row_sums = [jnp.sum(tiles_ref[k], axis=1, keepdims=True) for k in range(n_tile)]
    for k in range(n_tile):
        part[k] = row_sums[k] * rel_rows[k]

    def y_copy(off, c):
        return remote(
            ysend.at[off - 1, chunk[c]], yrecv.at[off - 1, chunk[c]],
            ys_sem.at[off - 1, c], yr_sem.at[off - 1, c], "ent", peers[off],
        )

    def z_copy(c):
        return remote(
            states_ref.at[chunk[c]], st.at[chunk[c]], zs_sem.at[c], zr_sem.at[c], "tm", up
        )

    def project(c, pieces):
        proj[0, chunk[c]] = dot3(pieces, both(wg))
        proj[1, chunk[c]] = dot3(pieces, both(ws))

    for c in range(CHUNKS):

        @pl.when(has_down)
        def _():
            z_copy(c).wait_recv()

        pieces = split(st[chunk[c]])
        if c < CHUNKS - 1:
            for k in range(n_tile):
                part[k] += dot3(both((th, tl), k, slice(None), chunk[c]), pieces)
            project(c, pieces)
        else:
            for d in range(CHUNKS):
                done = [
                    part[k, chunk[d]] + dot3(both((th, tl), k, chunk[d], chunk[c]), pieces)
                    for k in range(n_tile)
                ]
                for off in range(1, n_ent):
                    ysend[off - 1, chunk[d]] = sum(
                        done[k] * hits[off][k] for k in range(n_tile)
                    )
                    y_copy(off, d).start()
                agg[chunk[d]] = sum(done[k] * hits[0][k] for k in range(n_tile))
            project(c, pieces)

    for c in range(CHUNKS):
        total = agg[chunk[c]]
        for off in range(1, n_ent):
            y_copy(off, c).wait_recv()
            total = total + yrecv[off - 1, chunk[c]]
        agg[chunk[c]] = total
        u = jax.nn.sigmoid(proj[0, chunk[c]] + bias_ref[...])
        v = jnp.tanh(dot3(split(total), both(wn)) + proj[1, chunk[c]])
        states_ref[chunk[c]] = u * v + (1.0 - u) * st[chunk[c]]

        @pl.when(has_up)
        def _():
            z_copy(c).start()

        upd[chunk[c]] = u
        cand[chunk[c]] = v

    for k in range(n_tile):
        turned = tiles_ref[k].T
        sums = jnp.sum(turned, axis=0, keepdims=True)
        tth[k], ttl[k] = split(turned)
        for off in range(n_ent):
            target = msg_in if off == 0 else msg_out
            target[off, k : k + 1] = sums * hits[off][k]
            target[off, n_tile + k : n_tile + k + 1] = jnp.full_like(
                sums, rel_ref[k].astype(f32)
            )
    for off in range(n_ent):
        target = msg_in if off == 0 else msg_out
        if target.shape[1] > 2 * n_tile:
            target[off, 2 * n_tile :] = jnp.zeros(
                (target.shape[1] - 2 * n_tile, target.shape[2]), f32
            )

    def m_copy(off):
        return remote(
            msg_out.at[off], msg_in.at[off], ms_sem.at[off - 1], mr_sem.at[off - 1],
            "ent", peers[off],
        )

    for off in range(1, n_ent):
        m_copy(off).start()
    sth[...], stl[...] = split(st[...].T)
    agh[...], agl[...] = split(agg[...].T)
    u, v = upd[...], cand[...]
    coef_a[...] = u * (1.0 - v * v)
    coef_b[...] = (v - st[...]) * u * (1.0 - u)

    def g_copy(off, c):
        return remote(
            dagg.at[chunk[c]], grecv.at[off - 1, chunk[c]],
            gs_sem.at[off - 1, c], gr_sem.at[off - 1, c], "ent", peers[off],
        )

    def b_copy(c):
        return remote(dout.at[chunk[c]], dz.at[chunk[c]], bs_sem.at[c], br_sem.at[c], "tm", down)

    for c in range(CHUNKS):

        @pl.when(has_up)
        def _():
            b_copy(c).wait_recv()

        dnew = dz[chunk[c]] + cot_ref[chunk[c]]
        pre = dnew * coef_a[chunk[c]]
        gate = dnew * coef_b[chunk[c]]
        pre_pieces = split(pre)
        dagg[chunk[c]] = dot3(pre_pieces, both(wn), NT)

        @pl.when(has_down)
        def _():
            for off in range(1, n_ent):
                g_copy(off, c).start()

        dpre[chunk[c]] = pre
        dgate[chunk[c]] = gate

        @pl.when(has_down)
        def _():
            dprev[chunk[c]] = (
                dnew * (1.0 - upd[chunk[c]])
                + dot3(pre_pieces, both(ws), NT)
                + dot3(split(gate), both(wg), NT)
            )

    @pl.when(has_down)
    def _():
        for c in range(CHUNKS):
            own = dagg[chunk[c]]
            spread = [own * hits[0][k] for k in range(n_tile)]
            for off in range(1, n_ent):
                g_copy(off, c).wait_recv()
                other = grecv[off - 1, chunk[c]]
                for k in range(n_tile):
                    spread[k] = spread[k] + other * hits[n_ent - off][k]
            pieces = [split(spread[k]) for k in range(n_tile)]
            if c < CHUNKS - 1:
                dprev[...] += sum(
                    dot3(both((tth, ttl), k, slice(None), chunk[c]), pieces[k])
                    for k in range(n_tile)
                )
            else:
                for d in range(CHUNKS):
                    dout[chunk[d]] = dprev[chunk[d]] + sum(
                        dot3(both((tth, ttl), k, chunk[d], chunk[c]), pieces[k])
                        for k in range(n_tile)
                    )
                    b_copy(d).start()

    pre_pieces, gate_pieces = split(dpre[...]), split(dgate[...])
    n_rel = grel_ref.shape[0]
    base = [n_rel + width * i for i in range(4)]
    grads[base[0] : base[1]] = dot3(both((agh, agl)), pre_pieces)
    grads[base[1] : base[2]] = dot3(both((sth, stl)), pre_pieces)
    grads[base[2] : base[3]] = dot3(both((sth, stl)), gate_pieces)
    grads[base[3] :] = jnp.zeros((grads.shape[0] - base[3], width), f32)
    grads[base[3] : base[3] + 1] = jnp.sum(dgate[...], axis=0, keepdims=True)
    grad_pieces = split(dagg[...])
    number = lax.broadcasted_iota(jnp.int32, grel_ref.shape, 0).astype(f32)
    grad_rel = jnp.zeros(grel_ref.shape, f32)
    for off in range(n_ent):
        if off > 0:
            m_copy(off).wait_recv()
        found = dot3(split(msg_in[off]), grad_pieces)
        for k in range(n_tile):
            place = msg_in[off, n_tile + k : n_tile + k + 1, 0:1]
            grad_rel = grad_rel + jnp.where(number == place, found[k : k + 1], 0.0)
    grads[:n_rel] = grad_rel

    def move(src, dst, send, recv, target):
        return pltpu.make_async_remote_copy(
            src_ref=src, dst_ref=dst, send_sem=send, recv_sem=recv,
            device_id=target, device_id_type=MESH,
        )

    half = members * size
    cross = move(
        grads.at[pl.ds(pl.multiple_of((1 - side) * half, 8), half)], pair_in,
        one_sem.at[0], one_sem.at[1], pair,
    )
    cross.start()
    cross.wait_recv()
    half_sum[...] = grads[pl.ds(pl.multiple_of(side * half, 8), half)] + pair_in[...]

    def shard(index):
        return pl.ds(pl.multiple_of(index * size, 8), size)

    def scatter(q):
        index, target = mate(q)
        return move(
            half_sum.at[shard(index)], plane_in.at[q - 1], rs_sem.at[q - 1], rr_sem.at[q - 1],
            target,
        )

    for q in range(1, members):
        scatter(q).start()
    total = half_sum[shard(member)]
    for q in range(1, members):
        scatter(q).wait_recv()
        total = total + plane_in[q - 1]
    chain_out[...] = total
    chain = move(chain_out, chain_in, one_sem.at[2], one_sem.at[3], {"tm": down})

    @pl.when(has_up)
    def _():
        chain.wait_recv()
        chain_out[...] += chain_in[...]

    @pl.when(has_down)
    def _():
        chain.start()

    place = shard(side * members + member)

    def spread_copy(t):
        return move(
            final.at[place], final.at[place], cs_sem.at[t - 1], one_sem.at[4], {"tm": t}
        )

    @pl.when(tm == 0)
    def _():
        final[place] = chain_out[...]
        for t in range(n_tm - 1, 0, -1):
            spread_copy(t).start()

    @pl.when(has_down)
    def _():
        spread_copy(1).wait_recv()

    def gather(q, index):
        where = shard(side * members + index)
        return move(
            final.at[where], final.at[where], as_sem.at[q - 1], ar_sem.at[q - 1], mate(q)[1]
        )

    for q in range(1, members):
        gather(q, member).start()
    for q in range(1, members):
        gather(q, mate(-q)[0]).wait_recv()

    def swap(which):
        where = pl.ds(pl.multiple_of(which * half, 8), half)
        return move(final.at[where], final.at[where], one_sem.at[5], one_sem.at[6], pair)

    swap(side).start()
    swap(1 - side).wait_recv()
    grel_ref[...] = final[:n_rel]
    gneigh_ref[...] = final[base[0] : base[1]]
    gself_ref[...] = final[base[1] : base[2]]
    ggate_ref[...] = final[base[2] : base[3]]
    gbias_ref[...] = final[base[3] : base[3] + 1]

    cross.wait_send()
    swap(side).wait_send()
    for q in range(1, members):
        scatter(q).wait_send()
        gather(q, member).wait_send()

    @pl.when(has_down)
    def _():
        chain.wait_send()

    @pl.when(tm == 0)
    def _():
        for t in range(1, n_tm):
            spread_copy(t).wait_send()

    for off in range(1, n_ent):
        m_copy(off).wait_send()
        for c in range(CHUNKS):
            y_copy(off, c).wait_send()

    @pl.when(has_up)
    def _():
        for c in range(CHUNKS):
            z_copy(c).wait_send()

    @pl.when(has_down)
    def _():
        for c in range(CHUNKS):
            b_copy(c).wait_send()
            for off in range(1, n_ent):
                g_copy(off, c).wait_send()


def on_device(
    n_tm, n_ent, n_batch,
    init_state, tiles, dst_block, rel_id, cotangent, rel_emb, w_neigh, w_self, w_gate, b_gate
):
    assert tiles.shape[:2] == (1, 1)
    n_tile, rows = tiles.shape[2], tiles.shape[3]
    width, n_rel = init_state.shape[2], rel_emb.shape[0]
    lines = -(-2 * n_tile // 8) * 8
    others = max(n_ent - 1, 1)
    members = n_batch // 2 * n_ent
    shards = 2 * members
    size = -(-(n_rel + 3 * width + 8) // (8 * shards)) * 8
    mates = max(members - 1, 1)
    square, flat = (n_tile, rows, rows), (rows, width)
    vmem = pltpu.VMEM
    sems = pltpu.SemaphoreType.DMA
    whole, small = pl.BlockSpec(memory_space=pltpu.VMEM), pl.BlockSpec(memory_space=pltpu.SMEM)
    shape = lambda *dims: jax.ShapeDtypeStruct(dims, f32)
    weight = (width, width)
    outs = pl.pallas_call(
        functools.partial(step_kernel, n_tm, n_ent, n_batch),
        out_shape=(
            shape(rows, width), shape(n_rel, width), shape(*weight), shape(*weight),
            shape(*weight), shape(1, width),
        ),
        in_specs=[small, small] + [whole] * 8,
        out_specs=(whole,) * 6,
        scratch_shapes=[
            vmem(flat, f32), vmem(flat, f32), vmem(flat, f32), vmem(flat, f32),
            vmem(flat, f32), vmem(flat, f32), vmem((2,) + flat, f32),
            vmem((n_tile,) + flat, f32),
            vmem((others,) + flat, f32), vmem((others,) + flat, f32),
            vmem(flat, f32), vmem((others,) + flat, f32),
            vmem((n_ent, lines, rows), f32), vmem((n_ent, lines, rows), f32),
            vmem(square, bf16), vmem(square, bf16), vmem(square, bf16), vmem(square, bf16),
            vmem(weight, bf16), vmem(weight, bf16), vmem(weight, bf16), vmem(weight, bf16),
            vmem(weight, bf16), vmem(weight, bf16),
            vmem((width, rows), bf16), vmem((width, rows), bf16),
            vmem((width, rows), bf16), vmem((width, rows), bf16),
            vmem(flat, f32), vmem(flat, f32), vmem(flat, f32), vmem(flat, f32), vmem(flat, f32),
            vmem((shards * size, width), f32), vmem((members * size, width), f32),
            vmem((members * size, width), f32), vmem((mates, size, width), f32),
            vmem((size, width), f32), vmem((size, width), f32),
            vmem((shards * size, width), f32),
            sems((others, CHUNKS)), sems((others, CHUNKS)),
            sems((others, CHUNKS)), sems((others, CHUNKS)),
            sems((others,)), sems((others,)),
            sems((CHUNKS,)), sems((CHUNKS,)), sems((CHUNKS,)), sems((CHUNKS,)),
            sems((7,)), sems((mates,)), sems((mates,)), sems((n_tm,)),
            sems((mates,)), sems((mates,)),
        ],
        compiler_params=pltpu.CompilerParams(
            collective_id=0, has_side_effects=True, vmem_limit_bytes=60 * 1024 * 1024
        ),
    )(
        dst_block[0, 0], rel_id[0, 0], init_state[0], tiles[0, 0], cotangent[0, 0],
        rel_emb, w_neigh, w_self, w_gate, b_gate[None],
    )
    return (outs[0][None, None],) + tuple(outs[1:5]) + (outs[5][0],)


def solution(mesh):
    placed = (
        P("batch", "ent", None),
        P("batch", "tm", "ent", None, None),
        P("batch", "tm", "ent"),
        P("batch", "tm", "ent"),
        P("batch", "tm", "ent", None),
        P(),
        P(),
        P(),
        P(),
        P(),
    )
    return jax.shard_map(
        functools.partial(on_device, *(mesh.shape[name] for name in ("tm", "ent", "batch"))),
        mesh=mesh,
        in_specs=placed,
        out_specs=(P("batch", "tm", "ent", None), P(), P(), P(), P(), P()),
        check_vma=False,
    )
```

```python
import functools

import jax
import jax.numpy as jnp
from jax import lax
from jax.experimental import pallas as pl
from jax.experimental.pallas import tpu as pltpu
from jax.sharding import PartitionSpec as P

MESH = pl.DeviceIdType.MESH
CHUNKS = 4
PIECES = 8
f32, bf16 = jnp.float32, jnp.bfloat16
NN = (((1,), (0,)), ((), ()))
NT = (((1,), (1,)), ((), ()))


def split(value):
    high = value.astype(bf16)
    return high, (value - high.astype(f32)).astype(bf16)


def dot3(left, right, dims=NN):
    one = functools.partial(
        lax.dot_general, dimension_numbers=dims, preferred_element_type=f32
    )
    return one(left[0], right[0]) + (one(left[0], right[1]) + one(left[1], right[0]))


def remote(src, dst, send, recv, axis, index):
    return pltpu.make_async_remote_copy(
        src_ref=src, dst_ref=dst, send_sem=send, recv_sem=recv,
        device_id={axis: index}, device_id_type=MESH,
    )


def step_kernel(
    n_tm, n_ent, n_batch,
    dst_ref, rel_ref, init_ref, tiles_ref, cot_ref, emb_ref, wn_ref, ws_ref, wg_ref, bias_ref,
    states_ref, grel_ref, gneigh_ref, gself_ref, ggate_ref, gbias_ref,
    st, dz, dout, agg, upd, cand, proj, part, ysend, yrecv, dagg, grecv, msg_out, msg_in,
    th, tl, tth, ttl, wnh, wnl, wsh, wsl, wgh, wgl, sth, stl, agh, agl, coef_a, coef_b,
    dpre, dgate, dprev,
    grads, pair_in, half_sum, plane_in, chain_in, chain_out, final,
    ys_sem, yr_sem, gs_sem, gr_sem, ms_sem, mr_sem, zs_sem, zr_sem, bs_sem, br_sem,
    one_sem, rs_sem, rr_sem, cs_sem, as_sem, ar_sem,
):
    tm = lax.axis_index("tm")
    ent = lax.axis_index("ent")
    n_tile = tiles_ref.shape[0]
    rows, width = init_ref.shape
    step = rows // CHUNKS
    chunk = [slice(c * step, (c + 1) * step) for c in range(CHUNKS)]
    fine = rows // PIECES
    piece = [slice(p * fine, (p + 1) * fine) for p in range(PIECES)]
    inside = [range(c * PIECES // CHUNKS, (c + 1) * PIECES // CHUNKS) for c in range(CHUNKS)]
    peers = [lax.rem(ent + off, n_ent) for off in range(n_ent)]
    up = jnp.minimum(tm + 1, n_tm - 1)
    down = jnp.maximum(tm - 1, 0)
    has_up, has_down = tm < n_tm - 1, tm > 0

    batch = lax.axis_index("batch")
    side = lax.rem(batch, 2)
    pair = {"batch": batch + 1 - 2 * side}
    members = n_batch // 2 * n_ent
    member = batch // 2 * n_ent + ent
    size = plane_in.shape[1]

    def mate(distance):
        index = lax.rem(member + distance + members, members)
        return index, {"batch": index // n_ent * 2 + side, "ent": lax.rem(index, n_ent)}

    barrier = pltpu.get_barrier_semaphore()
    for q in range(1, members):
        pl.semaphore_signal(barrier, inc=1, device_id=mate(q)[1], device_id_type=MESH)
    pl.semaphore_signal(barrier, inc=1, device_id=pair, device_id_type=MESH)
    for q in range(1, n_tm):
        pl.semaphore_signal(
            barrier, inc=1, device_id={"tm": lax.rem(tm + q, n_tm)}, device_id_type=MESH
        )

    for k in range(n_tile):
        th[k], tl[k] = split(tiles_ref[k])
    wnh[...], wnl[...] = split(wn_ref[...])
    wsh[...], wsl[...] = split(ws_ref[...])
    wgh[...], wgl[...] = split(wg_ref[...])
    wn, ws, wg = (wnh, wnl), (wsh, wsl), (wgh, wgl)

    def both(pair, *index):
        return tuple(ref[index] if index else ref[...] for ref in pair)

    @pl.when(tm == 0)
    def _():
        st[...] = init_ref[...]

    @pl.when(tm == n_tm - 1)
    def _():
        dz[...] = jnp.zeros_like(dz)

    pl.semaphore_wait(barrier, members + n_tm - 1)

    hits = [
        [(dst_ref[k] == peers[off]).astype(f32) for k in range(n_tile)] for off in range(n_ent)
    ]
    rel_rows = [emb_ref[pl.ds(rel_ref[k], 1), :] for k in range(n_tile)]
    row_sums = [jnp.sum(tiles_ref[k], axis=1, keepdims=True) for k in range(n_tile)]
    for k in range(n_tile):
        part[k] = row_sums[k] * rel_rows[k]

    def y_copy(off, c):
        return remote(
            ysend.at[off - 1, piece[c]], yrecv.at[off - 1, piece[c]],
            ys_sem.at[off - 1, c], yr_sem.at[off - 1, c], "ent", peers[off],
        )

    def z_copy(c):
        return remote(
            states_ref.at[piece[c]], st.at[piece[c]], zs_sem.at[c], zr_sem.at[c], "tm", up
        )

    def project(c, pieces):
        proj[0, chunk[c]] = dot3(pieces, both(wg))
        proj[1, chunk[c]] = dot3(pieces, both(ws))

    for c in range(CHUNKS):

        @pl.when(has_down)
        def _():
            for p in inside[c]:
                z_copy(p).wait_recv()

        pieces = split(st[chunk[c]])
        if c < CHUNKS - 1:
            for k in range(n_tile):
                part[k] += dot3(both((th, tl), k, slice(None), chunk[c]), pieces)
            project(c, pieces)
        else:
            for d in range(PIECES):
                done = [
                    part[k, piece[d]] + dot3(both((th, tl), k, piece[d], chunk[c]), pieces)
                    for k in range(n_tile)
                ]
                for off in range(1, n_ent):
                    ysend[off - 1, piece[d]] = sum(
                        done[k] * hits[off][k] for k in range(n_tile)
                    )
                    y_copy(off, d).start()
                agg[piece[d]] = sum(done[k] * hits[0][k] for k in range(n_tile))
            project(c, pieces)

    for c in range(PIECES):
        total = agg[piece[c]]
        for off in range(1, n_ent):
            y_copy(off, c).wait_recv()
            total = total + yrecv[off - 1, piece[c]]
        agg[piece[c]] = total
        u = jax.nn.sigmoid(proj[0, piece[c]] + bias_ref[...])
        v = jnp.tanh(dot3(split(total), both(wn)) + proj[1, piece[c]])
        states_ref[piece[c]] = u * v + (1.0 - u) * st[piece[c]]

        @pl.when(has_up)
        def _():
            z_copy(c).start()

        upd[piece[c]] = u
        cand[piece[c]] = v

    for k in range(n_tile):
        turned = tiles_ref[k].T
        sums = jnp.sum(turned, axis=0, keepdims=True)
        tth[k], ttl[k] = split(turned)
        for off in range(n_ent):
            target = msg_in if off == 0 else msg_out
            target[off, k : k + 1] = sums * hits[off][k]
            target[off, n_tile + k : n_tile + k + 1] = jnp.full_like(
                sums, rel_ref[k].astype(f32)
            )
    for off in range(n_ent):
        target = msg_in if off == 0 else msg_out
        if target.shape[1] > 2 * n_tile:
            target[off, 2 * n_tile :] = jnp.zeros(
                (target.shape[1] - 2 * n_tile, target.shape[2]), f32
            )

    def m_copy(off):
        return remote(
            msg_out.at[off], msg_in.at[off], ms_sem.at[off - 1], mr_sem.at[off - 1],
            "ent", peers[off],
        )

    for off in range(1, n_ent):
        m_copy(off).start()
    sth[...], stl[...] = split(st[...].T)
    agh[...], agl[...] = split(agg[...].T)
    u, v = upd[...], cand[...]
    coef_a[...] = u * (1.0 - v * v)
    coef_b[...] = (v - st[...]) * u * (1.0 - u)

    def g_copy(off, c):
        return remote(
            dagg.at[piece[c]], grecv.at[off - 1, piece[c]],
            gs_sem.at[off - 1, c], gr_sem.at[off - 1, c], "ent", peers[off],
        )

    def b_copy(c):
        return remote(dout.at[piece[c]], dz.at[piece[c]], bs_sem.at[c], br_sem.at[c], "tm", down)

    for c in range(PIECES):

        @pl.when(has_up)
        def _():
            b_copy(c).wait_recv()

        dnew = dz[piece[c]] + cot_ref[piece[c]]
        pre = dnew * coef_a[piece[c]]
        gate = dnew * coef_b[piece[c]]
        pre_pieces = split(pre)
        dagg[piece[c]] = dot3(pre_pieces, both(wn), NT)

        @pl.when(has_down)
        def _():
            for off in range(1, n_ent):
                g_copy(off, c).start()

        dpre[piece[c]] = pre
        dgate[piece[c]] = gate

        @pl.when(has_down)
        def _():
            dprev[piece[c]] = (
                dnew * (1.0 - upd[piece[c]])
                + dot3(pre_pieces, both(ws), NT)
                + dot3(split(gate), both(wg), NT)
            )

    @pl.when(has_down)
    def _():
        for c in range(CHUNKS):
            own = dagg[chunk[c]]
            spread = [own * hits[0][k] for k in range(n_tile)]
            for off in range(1, n_ent):
                for p in inside[c]:
                    g_copy(off, p).wait_recv()
                other = grecv[off - 1, chunk[c]]
                for k in range(n_tile):
                    spread[k] = spread[k] + other * hits[n_ent - off][k]
            pieces = [split(spread[k]) for k in range(n_tile)]
            if c < CHUNKS - 1:
                dprev[...] += sum(
                    dot3(both((tth, ttl), k, slice(None), chunk[c]), pieces[k])
                    for k in range(n_tile)
                )
            else:
                for d in range(PIECES):
                    dout[piece[d]] = dprev[piece[d]] + sum(
                        dot3(both((tth, ttl), k, piece[d], chunk[c]), pieces[k])
                        for k in range(n_tile)
                    )
                    b_copy(d).start()

    pre_pieces, gate_pieces = split(dpre[...]), split(dgate[...])
    n_rel = grel_ref.shape[0]
    base = [n_rel + width * i for i in range(4)]
    grads[base[0] : base[1]] = dot3(both((agh, agl)), pre_pieces)
    grads[base[1] : base[2]] = dot3(both((sth, stl)), pre_pieces)
    grads[base[2] : base[3]] = dot3(both((sth, stl)), gate_pieces)
    grads[base[3] :] = jnp.zeros((grads.shape[0] - base[3], width), f32)
    grads[base[3] : base[3] + 1] = jnp.sum(dgate[...], axis=0, keepdims=True)
    grad_pieces = split(dagg[...])
    number = lax.broadcasted_iota(jnp.int32, grel_ref.shape, 0).astype(f32)
    grad_rel = jnp.zeros(grel_ref.shape, f32)
    for off in range(n_ent):
        if off > 0:
            m_copy(off).wait_recv()
        found = dot3(split(msg_in[off]), grad_pieces)
        for k in range(n_tile):
            place = msg_in[off, n_tile + k : n_tile + k + 1, 0:1]
            grad_rel = grad_rel + jnp.where(number == place, found[k : k + 1], 0.0)
    grads[:n_rel] = grad_rel

    def move(src, dst, send, recv, target):
        return pltpu.make_async_remote_copy(
            src_ref=src, dst_ref=dst, send_sem=send, recv_sem=recv,
            device_id=target, device_id_type=MESH,
        )

    half = members * size
    cross = move(
        grads.at[pl.ds(pl.multiple_of((1 - side) * half, 8), half)], pair_in,
        one_sem.at[0], one_sem.at[1], pair,
    )
    cross.start()
    cross.wait_recv()
    half_sum[...] = grads[pl.ds(pl.multiple_of(side * half, 8), half)] + pair_in[...]

    def shard(index):
        return pl.ds(pl.multiple_of(index * size, 8), size)

    def scatter(q):
        index, target = mate(q)
        return move(
            half_sum.at[shard(index)], plane_in.at[q - 1], rs_sem.at[q - 1], rr_sem.at[q - 1],
            target,
        )

    for q in range(1, members):
        scatter(q).start()
    total = half_sum[shard(member)]
    for q in range(1, members):
        scatter(q).wait_recv()
        total = total + plane_in[q - 1]
    chain_out[...] = total
    chain = move(chain_out, chain_in, one_sem.at[2], one_sem.at[3], {"tm": down})

    @pl.when(has_up)
    def _():
        chain.wait_recv()
        chain_out[...] += chain_in[...]

    @pl.when(has_down)
    def _():
        chain.start()

    place = shard(side * members + member)

    def spread_copy(t):
        return move(
            final.at[place], final.at[place], cs_sem.at[t - 1], one_sem.at[4], {"tm": t}
        )

    @pl.when(tm == 0)
    def _():
        final[place] = chain_out[...]
        for t in range(n_tm - 1, 0, -1):
            spread_copy(t).start()

    @pl.when(has_down)
    def _():
        spread_copy(1).wait_recv()

    def gather(q, index):
        where = shard(side * members + index)
        return move(
            final.at[where], final.at[where], as_sem.at[q - 1], ar_sem.at[q - 1], mate(q)[1]
        )

    for q in range(1, members):
        gather(q, member).start()
    for q in range(1, members):
        gather(q, mate(-q)[0]).wait_recv()

    def swap(which):
        where = pl.ds(pl.multiple_of(which * half, 8), half)
        return move(final.at[where], final.at[where], one_sem.at[5], one_sem.at[6], pair)

    swap(side).start()
    swap(1 - side).wait_recv()
    grel_ref[...] = final[:n_rel]
    gneigh_ref[...] = final[base[0] : base[1]]
    gself_ref[...] = final[base[1] : base[2]]
    ggate_ref[...] = final[base[2] : base[3]]
    gbias_ref[...] = final[base[3] : base[3] + 1]

    cross.wait_send()
    swap(side).wait_send()
    for q in range(1, members):
        scatter(q).wait_send()
        gather(q, member).wait_send()

    @pl.when(has_down)
    def _():
        chain.wait_send()

    @pl.when(tm == 0)
    def _():
        for t in range(1, n_tm):
            spread_copy(t).wait_send()

    for off in range(1, n_ent):
        m_copy(off).wait_send()
        for c in range(PIECES):
            y_copy(off, c).wait_send()

    @pl.when(has_up)
    def _():
        for c in range(PIECES):
            z_copy(c).wait_send()

    @pl.when(has_down)
    def _():
        for c in range(PIECES):
            b_copy(c).wait_send()
            for off in range(1, n_ent):
                g_copy(off, c).wait_send()


def on_device(
    n_tm, n_ent, n_batch,
    init_state, tiles, dst_block, rel_id, cotangent, rel_emb, w_neigh, w_self, w_gate, b_gate
):
    assert tiles.shape[:2] == (1, 1)
    n_tile, rows = tiles.shape[2], tiles.shape[3]
    width, n_rel = init_state.shape[2], rel_emb.shape[0]
    lines = -(-2 * n_tile // 8) * 8
    others = max(n_ent - 1, 1)
    members = n_batch // 2 * n_ent
    shards = 2 * members
    size = -(-(n_rel + 3 * width + 8) // (8 * shards)) * 8
    mates = max(members - 1, 1)
    square, flat = (n_tile, rows, rows), (rows, width)
    vmem = pltpu.VMEM
    sems = pltpu.SemaphoreType.DMA
    whole, small = pl.BlockSpec(memory_space=pltpu.VMEM), pl.BlockSpec(memory_space=pltpu.SMEM)
    shape = lambda *dims: jax.ShapeDtypeStruct(dims, f32)
    weight = (width, width)
    outs = pl.pallas_call(
        functools.partial(step_kernel, n_tm, n_ent, n_batch),
        out_shape=(
            shape(rows, width), shape(n_rel, width), shape(*weight), shape(*weight),
            shape(*weight), shape(1, width),
        ),
        in_specs=[small, small] + [whole] * 8,
        out_specs=(whole,) * 6,
        scratch_shapes=[
            vmem(flat, f32), vmem(flat, f32), vmem(flat, f32), vmem(flat, f32),
            vmem(flat, f32), vmem(flat, f32), vmem((2,) + flat, f32),
            vmem((n_tile,) + flat, f32),
            vmem((others,) + flat, f32), vmem((others,) + flat, f32),
            vmem(flat, f32), vmem((others,) + flat, f32),
            vmem((n_ent, lines, rows), f32), vmem((n_ent, lines, rows), f32),
            vmem(square, bf16), vmem(square, bf16), vmem(square, bf16), vmem(square, bf16),
            vmem(weight, bf16), vmem(weight, bf16), vmem(weight, bf16), vmem(weight, bf16),
            vmem(weight, bf16), vmem(weight, bf16),
            vmem((width, rows), bf16), vmem((width, rows), bf16),
            vmem((width, rows), bf16), vmem((width, rows), bf16),
            vmem(flat, f32), vmem(flat, f32), vmem(flat, f32), vmem(flat, f32), vmem(flat, f32),
            vmem((shards * size, width), f32), vmem((members * size, width), f32),
            vmem((members * size, width), f32), vmem((mates, size, width), f32),
            vmem((size, width), f32), vmem((size, width), f32),
            vmem((shards * size, width), f32),
            sems((others, PIECES)), sems((others, PIECES)),
            sems((others, PIECES)), sems((others, PIECES)),
            sems((others,)), sems((others,)),
            sems((PIECES,)), sems((PIECES,)), sems((PIECES,)), sems((PIECES,)),
            sems((7,)), sems((mates,)), sems((mates,)), sems((n_tm,)),
            sems((mates,)), sems((mates,)),
        ],
        compiler_params=pltpu.CompilerParams(
            collective_id=0, has_side_effects=True, vmem_limit_bytes=60 * 1024 * 1024
        ),
    )(
        dst_block[0, 0], rel_id[0, 0], init_state[0], tiles[0, 0], cotangent[0, 0],
        rel_emb, w_neigh, w_self, w_gate, b_gate[None],
    )
    return (outs[0][None, None],) + tuple(outs[1:5]) + (outs[5][0],)


def solution(mesh):
    placed = (
        P("batch", "ent", None),
        P("batch", "tm", "ent", None, None),
        P("batch", "tm", "ent"),
        P("batch", "tm", "ent"),
        P("batch", "tm", "ent", None),
        P(),
        P(),
        P(),
        P(),
        P(),
    )
    return jax.shard_map(
        functools.partial(on_device, *(mesh.shape[name] for name in ("tm", "ent", "batch"))),
        mesh=mesh,
        in_specs=placed,
        out_specs=(P("batch", "tm", "ent", None), P(), P(), P(), P(), P()),
        check_vma=False,
    )
```
